32 devices in a mesh: head: 4 (over y, core), ctx: 8 (over z, x).
Axes of the slice: x: 2, y: 2, z: 4, core: 2. Of those that a mesh axis runs over, the one named last changes fastest.
Arguments:
- queries: bfloat16 [6144, 4, 1024], P('ctx', 'head'), may hold values from -200 to 200
- keys: bfloat16 [6144, 4, 128], P('ctx', 'head'), may hold values from -6 to 6
- values: bfloat16 [6144, 4, 128], P('ctx', 'head'), may hold values from -6 to 6
- span_ids: int32 [16], replicated, may hold values from 0 to 15, as said below
Outputs:
- attn_out: bfloat16 [6144, 4, 1024], P('ctx', 'head')
The draws below stay inside these ranges and needn't reach their ends.
Inputs may be any that keep to these rules, and one draw needn't show every extreme that they name: `span_ids`: entry 2r is below 8, entry 2r + 1 equals 15 minus entry 2r, and all entries differ.
All inputs are finite; a program needn't handle non-finite values.
Results may differ from the reference program's by a relative error of at most 0.0055.
Values may be sent and summed in bfloat16 or wider, within the bound.
A program may use at most 64 MiB of HBM per device.

```python
import jax
import jax.numpy as jnp
from jax import lax

HD = 128
GRP = 8
KVH = 4
CH = 384
NCHUNK = 16
TOKENS = 6144
N_CTX = 8


def drawn(key):
    base_keys = jnp.clip(jax.random.normal(jax.random.fold_in(key, 11), (TOKENS, KVH, HD), jnp.float32), -6.0, 6.0)
    return base_keys


def draw_keys(key, part):
    base_keys = drawn(key)
    return base_keys.astype(jnp.bfloat16)


def draw_queries(key, part):
    base = jnp.clip(jax.random.normal(jax.random.fold_in(key, 21), (TOKENS, KVH, GRP * HD), jnp.float32), -6.0, 6.0)
    return base.astype(jnp.bfloat16)


def draw_span_ids(key, part):
    order = jax.random.permutation(jax.random.fold_in(key, 31), N_CTX).astype(jnp.int32)
    return jnp.stack([order, NCHUNK - 1 - order], axis=1).reshape(NCHUNK).astype(jnp.int32)


def block_scale(rng, shape, pieces, low, high):
    def one(position, blocks):
        heights = jax.random.uniform(jax.random.fold_in(jax.random.fold_in(rng, 6), position), (blocks,), jnp.float32, low / len(pieces), high / len(pieces))
        return jnp.repeat(jnp.exp(heights), shape[position] // blocks).reshape((-1,) + (1,) * (len(shape) - position - 1))

    factor_of = one(*pieces[0])
    for cut in pieces[1:]:
        factor_of = factor_of * one(*cut)
    return factor_of


def normal_values(own_key, shape, deviation, most, pieces=(), kind=jnp.bfloat16):
    drawn = deviation * jax.random.normal(own_key, shape, jnp.float32)
    if pieces:
        drawn = drawn * block_scale(own_key, shape, pieces, -0.22, 0.18)
    return jnp.clip(drawn, -most, most).astype(kind)


def setup_inputs(seed: int = 0) -> dict:
    key_of = jax.random.split(jax.random.key(seed), 5)
    return {
        "queries": draw_queries(jax.random.fold_in(key_of[4], 71), 0),
        "keys": draw_keys(jax.random.fold_in(key_of[4], 71), 0),
        "values": normal_values(key_of[2], (TOKENS, KVH, HD), 1.0, 6.0, ((0, 8), (1, 4))),
        "span_ids": draw_span_ids(jax.random.fold_in(key_of[4], 71), 0),
    }


def reference(queries, keys, values, span_ids):
    tokens = queries.shape[0]
    row_ids = jnp.arange(tokens, dtype=jnp.int32)
    positions = (jnp.take(span_ids, row_ids // CH) * CH + row_ids % CH).astype(jnp.int32)
    score_scale = HD ** -0.5
    query_all = jnp.moveaxis(queries.reshape(tokens, KVH, GRP, HD), 1, 0)
    key_all = jnp.moveaxis(keys, 1, 0)
    value_all = jnp.moveaxis(values, 1, 0)

    def one_head(inputs_now):
        query_head, key_head, value_head = inputs_now
        key_float = key_head.astype(jnp.float32)
        value_float = value_head.astype(jnp.float32)
        query_blocks = query_head.reshape(tokens // CH, CH, GRP, HD)
        block_pos = positions.reshape(tokens // CH, CH)

        def one_block(block_now):
            query_block, query_pos = block_now
            scores = jnp.einsum("qgd,kd->qgk", query_block.astype(jnp.float32), key_float,
                                precision=lax.Precision.HIGHEST) * score_scale
            allowed = positions[None, None, :] <= query_pos[:, None, None]
            scores = jnp.where(allowed, scores, -1e30)
            row_max = jnp.max(scores, axis=2, keepdims=True)
            weights = jnp.where(allowed, jnp.exp(scores - row_max), 0.0)
            weight_sum = jnp.sum(weights, axis=2)
            rounded = lax.optimization_barrier(weights.astype(jnp.bfloat16)).astype(jnp.float32)
            mixed = jnp.einsum("qgk,kd->qgd", rounded, value_float, precision=lax.Precision.HIGHEST)
            return (mixed / weight_sum[:, :, None]).astype(jnp.bfloat16)

        return lax.map(one_block, (query_blocks, block_pos)).reshape(tokens, GRP * HD)

    result = lax.map(one_head, (query_all, key_all, value_all))
    return jnp.moveaxis(result, 0, 1)
```

```python
import functools
import math

import jax
import jax.numpy as jnp
from jax import lax
from jax.experimental import pallas as pl
from jax.experimental.pallas import tpu as pltpu
from jax.sharding import PartitionSpec as P

MESH = pl.DeviceIdType.MESH
LOW, HIGH = 0, 1
TO_PARTNER, TO_NEXT, TO_PREV = 0, 1, 2
MASKED = -1e30
HEADS_PER_STEP = 2


def kernel(
    count, head_dim, ids, q_hbm, k_hbm, v_hbm, o_hbm,
    q, kv, kv_pick, acc, top, total, out, in_sem, out_sem, send_sem, recv_sem,
):
    groups, rows, _ = q.shape
    span = rows // 2
    line = count // 2
    lanes = head_dim
    pieces = span // lanes
    scale = head_dim ** (-0.5) * math.log2(math.e)
    me = lax.axis_index("ctx")
    z = me // 2
    x = me % 2
    partner = z * 2 + 1 - x

    def kv_in(half, which, src):
        return pltpu.make_async_copy(
            src.at[pl.ds(half * span, span), :], kv.at[me, half, which], in_sem.at[half, which]
        )

    def q_in(group):
        return pltpu.make_async_copy(
            q_hbm.at[:, pl.ds(group * lanes, lanes)], q.at[group], in_sem.at[2 + group, 0]
        )

    for half in range(2):
        kv_in(half, 0, k_hbm).start()
        kv_in(half, 1, v_hbm).start()
    for group in range(groups):
        q_in(group).start()

    barrier = pltpu.get_barrier_semaphore()
    pl.semaphore_signal(barrier, inc=1, device_id={"ctx": partner}, device_id_type=MESH)

    @pl.when(z > 0)
    def _():
        pl.semaphore_signal(barrier, inc=1, device_id={"ctx": me - 2}, device_id_type=MESH)

    @pl.when(z < line - 1)
    def _():
        pl.semaphore_signal(barrier, inc=1, device_id={"ctx": me + 2}, device_id_type=MESH)

    near = 1 + jnp.where(z > 0, 1, 0) + jnp.where(z < line - 1, 1, 0)
    pl.semaphore_wait(barrier, near)

    def sent(owner, half, way):
        target = (partner, me + 2, me - 2)[way]
        return pltpu.make_async_remote_copy(
            src_ref=kv.at[owner, half],
            dst_ref=kv.at[owner, half],
            send_sem=send_sem.at[owner, half, way],
            recv_sem=recv_sem.at[owner, half],
            device_id={"ctx": target},
            device_id_type=MESH,
        )

    for half in range(2):
        kv_in(half, 0, k_hbm).wait()
        kv_in(half, 1, v_hbm).wait()

        @pl.when(z < line - 1)
        def _():
            sent(me, half, TO_NEXT).start()

        @pl.when(z > 0)
        def _():
            sent(me, half, TO_PREV).start()

        sent(me, half, TO_PARTNER).start()

    def relay(step, half):
        before = z - step
        after = z + step

        @pl.when(before >= 0)
        def _():
            owner = before * 2 + x
            sent(owner, half, TO_PARTNER).wait_recv()

            @pl.when(z < line - 1)
            def _():
                sent(owner, half, TO_NEXT).start()

            sent(owner, half, TO_PARTNER).start()

        @pl.when(after < line)
        def _():
            owner = after * 2 + x
            sent(owner, half, TO_PARTNER).wait_recv()

            @pl.when(z > 0)
            def _():
                sent(owner, half, TO_PREV).start()

            sent(owner, half, TO_PARTNER).start()

    for group in range(groups):
        q_in(group).wait()

    def score(q_part, k_part):
        return lax.dot_general(
            q_part, k_part, (((1,), (1,)), ((), ())), preferred_element_type=jnp.float32
        )

    def row_top(s):
        best = s[:, :lanes]
        for piece in range(1, pieces):
            best = jnp.maximum(best, s[:, piece * lanes : (piece + 1) * lanes])
        return jnp.max(best, axis=1, keepdims=True)

    def weigh(s, m):
        parts = [
            jnp.exp2((s[:, piece * lanes : (piece + 1) * lanes] - m) * scale)
            for piece in range(pieces)
        ]
        summed = parts[0]
        for part in parts[1:]:
            summed = summed + part
        return jnp.concatenate([part.astype(jnp.bfloat16) for part in parts], axis=1), summed

    def mix(p, v_part):
        return jnp.dot(p, v_part, preferred_element_type=jnp.float32)

    def over_groups(body):
        def step(index, carry):
            for inner in range(HEADS_PER_STEP):
                body(index * HEADS_PER_STEP + inner)
            return carry

        lax.fori_loop(0, groups // HEADS_PER_STEP, step, 0)

    def half_q(group, half):
        return q[group, half * span : (half + 1) * span, :]

    def own_span(half):
        row_no = lax.broadcasted_iota(jnp.int32, (span, span), 0)
        key_no = lax.broadcasted_iota(jnp.int32, (span, span), 1)

        def body(group):
            s = score(half_q(group, half), kv[me, half, 0])
            s = jnp.where(key_no <= row_no, s, MASKED)
            m = jnp.broadcast_to(row_top(s), (span, lanes))
            p, summed = weigh(s, m)
            top[half, group] = m
            total[half, group] = summed
            acc[half, group] = mix(p, kv[me, half, 1])

        over_groups(body)

    def high_on_low(owner):
        def body(group):
            s = score(half_q(group, HIGH), kv[owner, LOW, 0])
            old = top[HIGH, group]
            m = jnp.maximum(old, row_top(s))
            fade = jnp.exp2((old - m) * scale)
            p, summed = weigh(s, m)
            top[HIGH, group] = m
            total[HIGH, group] = total[HIGH, group] * fade + summed
            acc[HIGH, group] = acc[HIGH, group] * fade + mix(p, kv[owner, LOW, 1])

        over_groups(body)

    def same_half(owner):
        flag = jnp.where(ids[2 * owner] > ids[2 * me], 1, 0)
        is_high = jnp.full((span, lanes), flag, jnp.int32) == 1
        for which in range(2):
            kv_pick[which] = jnp.where(is_high, kv[owner, HIGH, which], kv[owner, LOW, which])

        def body(group):
            s = score(jnp.where(is_high, half_q(group, HIGH), half_q(group, LOW)), kv_pick[0])
            tops = [top[half, group] for half in range(2)]
            old = jnp.where(is_high, tops[HIGH], tops[LOW])
            m = jnp.maximum(old, row_top(s))
            fade = jnp.exp2((old - m) * scale)
            p, summed = weigh(s, m)
            top[LOW, group] = jnp.where(is_high, tops[LOW], m)
            top[HIGH, group] = jnp.where(is_high, m, tops[HIGH])
            added = mix(p, kv_pick[1])
            for ref, extra in ((total, summed), (acc, added)):
                low_now, high_now = ref[LOW, group], ref[HIGH, group]
                new = jnp.where(is_high, high_now, low_now) * fade + extra
                ref[LOW, group] = jnp.where(is_high, low_now, new)
                ref[HIGH, group] = jnp.where(is_high, new, high_now)

        over_groups(body)

    own_span(LOW)
    own_span(HIGH)
    high_on_low(me)

    short = jnp.minimum(z, line - 1 - z)
    far_side = jnp.where(z <= line - 1 - z, 1, -1)

    def line_place(order):
        paired = jnp.where(order % 2 == 1, -1, 1) * ((order + 1) // 2)
        alone = far_side * (order - short)
        return z + jnp.where(order <= 2 * short, paired, alone)

    def visit(index, carry):
        on_line = index % 2
        step = index // 2 + 1
        order = index // 2 + on_line
        owner = line_place(order) * 2 + jnp.where(on_line == 1, x, 1 - x)
        moving = jnp.logical_and(on_line == 0, step < line)
        for half in range(2):

            @pl.when(moving)
            def _():
                relay(step, half)

            @pl.when(on_line == 0)
            def _():
                sent(owner, half, TO_PARTNER).wait_recv()

            if half == LOW:
                high_on_low(owner)
            else:
                same_half(owner)
        return carry

    lax.fori_loop(0, count - 1, visit, 0)

    def finish(group):
        for half in range(2):
            weight = jnp.sum(total[half, group], axis=1, keepdims=True)
            out[group, half * span : (half + 1) * span, :] = (
                acc[half, group] / weight
            ).astype(out.dtype)

    def result(group):
        return pltpu.make_async_copy(
            out.at[group], o_hbm.at[:, pl.ds(group * lanes, lanes)], out_sem.at[group]
        )

    for group in range(groups):
        finish(group)
        result(group).start()

    def settle(place, carry):
        owner = place * 2 + x
        for half in range(2):
            sent(owner, half, TO_PARTNER).wait_send()

            @pl.when(jnp.logical_and(place <= z, z < line - 1))
            def _():
                sent(owner, half, TO_NEXT).wait_send()

            @pl.when(jnp.logical_and(place >= z, z > 0))
            def _():
                sent(owner, half, TO_PREV).wait_send()

        return carry

    lax.fori_loop(0, line, settle, 0)
    for group in range(groups):
        result(group).wait()


def local(count, queries, keys, values, span_ids):
    rows = queries.shape[0]
    head_dim = keys.shape[2]
    width = queries.shape[2]
    groups = width // head_dim
    span = rows // 2
    any_space = pl.BlockSpec(memory_space=pl.ANY)
    out = pl.pallas_call(
        functools.partial(kernel, count, head_dim),
        out_shape=jax.ShapeDtypeStruct((rows, width), jnp.bfloat16),
        in_specs=[pl.BlockSpec(memory_space=pltpu.SMEM), any_space, any_space, any_space],
        out_specs=any_space,
        scratch_shapes=[
            pltpu.VMEM((groups, rows, head_dim), jnp.bfloat16),
            pltpu.VMEM((count, 2, 2, span, head_dim), jnp.bfloat16),
            pltpu.VMEM((2, span, head_dim), jnp.bfloat16),
            pltpu.VMEM((2, groups, span, head_dim), jnp.float32),
            pltpu.VMEM((2, groups, span, head_dim), jnp.float32),
            pltpu.VMEM((2, groups, span, head_dim), jnp.float32),
            pltpu.VMEM((groups, rows, head_dim), jnp.bfloat16),
            pltpu.SemaphoreType.DMA((2 + groups, 2)),
            pltpu.SemaphoreType.DMA((groups,)),
            pltpu.SemaphoreType.DMA((count, 2, 3)),
            pltpu.SemaphoreType.DMA((count, 2)),
        ],
        compiler_params=pltpu.CompilerParams(
            collective_id=0, has_side_effects=True, vmem_limit_bytes=56 * 2**20
        ),
    )(
        span_ids,
        queries.reshape(rows, width),
        keys.reshape(rows, head_dim),
        values.reshape(rows, head_dim),
    )
    return out.reshape(rows, 1, width)


def solution(mesh):
    in_specs = (P("ctx", "head", None), P("ctx", "head", None), P("ctx", "head", None), P())
    out_specs = P("ctx", "head", None)
    body = functools.partial(local, mesh.shape["ctx"])
    return jax.shard_map(body, mesh=mesh, in_specs=in_specs, out_specs=out_specs, check_vma=False)
```

```python
import functools
import math

import jax
import jax.numpy as jnp
from jax import lax
from jax.experimental import pallas as pl
from jax.experimental.pallas import tpu as pltpu
from jax.sharding import PartitionSpec as P

MESH = pl.DeviceIdType.MESH
LOW, HIGH = 0, 1
TO_PARTNER, TO_NEXT, TO_PREV = 0, 1, 2
MASKED = -1e30
SLAB = 4
SLABS_PER_STEP = 1


def kernel(
    count, head_dim, ids, q_hbm, k_hbm, v_hbm, o_hbm,
    q, kv, kv_pick, acc, top, total, out, in_sem, out_sem, send_sem, recv_sem,
):
    groups, rows, _ = q.shape
    span = rows // 2
    line = count // 2
    lanes = head_dim
    slab = math.gcd(groups, SLAB)
    per_step = math.gcd(groups // slab, SLABS_PER_STEP)
    tall = slab * span
    scale = head_dim ** (-0.5) * math.log2(math.e)
    me = lax.axis_index("ctx")
    z = me // 2
    x = me % 2
    partner = z * 2 + 1 - x

    def kv_in(half, which, src):
        return pltpu.make_async_copy(
            src.at[pl.ds(half * span, span), :], kv.at[me, half, which], in_sem.at[half, which]
        )

    def q_in(group):
        return pltpu.make_async_copy(
            q_hbm.at[:, pl.ds(group * lanes, lanes)], q.at[group], in_sem.at[2 + group, 0]
        )

    for half in range(2):
        kv_in(half, 0, k_hbm).start()
        kv_in(half, 1, v_hbm).start()
    for group in range(groups):
        q_in(group).start()

    barrier = pltpu.get_barrier_semaphore()
    pl.semaphore_signal(barrier, inc=1, device_id={"ctx": partner}, device_id_type=MESH)

    @pl.when(z > 0)
    def _():
        pl.semaphore_signal(barrier, inc=1, device_id={"ctx": me - 2}, device_id_type=MESH)

    @pl.when(z < line - 1)
    def _():
        pl.semaphore_signal(barrier, inc=1, device_id={"ctx": me + 2}, device_id_type=MESH)

    near = 1 + jnp.where(z > 0, 1, 0) + jnp.where(z < line - 1, 1, 0)
    pl.semaphore_wait(barrier, near)

    def sent(owner, half, way):
        target = (partner, me + 2, me - 2)[way]
        return pltpu.make_async_remote_copy(
            src_ref=kv.at[owner, half],
            dst_ref=kv.at[owner, half],
            send_sem=send_sem.at[owner, half, way],
            recv_sem=recv_sem.at[owner, half],
            device_id={"ctx": target},
            device_id_type=MESH,
        )

    for half in range(2):
        kv_in(half, 0, k_hbm).wait()
        kv_in(half, 1, v_hbm).wait()

        @pl.when(z < line - 1)
        def _():
            sent(me, half, TO_NEXT).start()

        @pl.when(z > 0)
        def _():
            sent(me, half, TO_PREV).start()

        sent(me, half, TO_PARTNER).start()

    def relay(step, half):
        before = z - step
        after = z + step

        @pl.when(before >= 0)
        def _():
            owner = before * 2 + x
            sent(owner, half, TO_PARTNER).wait_recv()

            @pl.when(z < line - 1)
            def _():
                sent(owner, half, TO_NEXT).start()

            sent(owner, half, TO_PARTNER).start()

        @pl.when(after < line)
        def _():
            owner = after * 2 + x
            sent(owner, half, TO_PARTNER).wait_recv()

            @pl.when(z > 0)
            def _():
                sent(owner, half, TO_PREV).start()

            sent(owner, half, TO_PARTNER).start()

    for group in range(groups):
        q_in(group).wait()

    def score(q_part, k_part):
        return lax.dot_general(
            q_part, k_part, (((1,), (1,)), ((), ())), preferred_element_type=jnp.float32
        )

    def row_top(s):
        best = s[:, :lanes]
        for piece in range(1, s.shape[1] // lanes):
            best = jnp.maximum(best, s[:, piece * lanes : (piece + 1) * lanes])
        return jnp.max(best, axis=1, keepdims=True)

    def weigh(s, m):
        parts = [
            jnp.exp2((s[:, piece * lanes : (piece + 1) * lanes] - m) * scale)
            for piece in range(s.shape[1] // lanes)
        ]
        summed = parts[0]
        for part in parts[1:]:
            summed = summed + part
        return jnp.concatenate([part.astype(jnp.bfloat16) for part in parts], axis=1), summed

    def mix(p, v_part):
        return jnp.dot(p, v_part, preferred_element_type=jnp.float32)

    def over_groups(body):
        def step(index, carry):
            for inner in range(per_step):
                body(pl.ds((index * per_step + inner) * slab, slab))
            return carry

        lax.fori_loop(0, groups // (slab * per_step), step, 0)

    def half_q(group, half):
        return q[group, half * span : (half + 1) * span, :].reshape(tall, lanes)

    def read(ref, half, group):
        return ref[half, group].reshape(tall, lanes)

    def write(ref, half, group, value):
        ref[half, group] = value.reshape(slab, span, lanes)

    def own_span(half):
        row_no = lax.broadcasted_iota(jnp.int32, (tall, span), 0) % span
        key_no = lax.broadcasted_iota(jnp.int32, (tall, span), 1)

        def body(group):
            s = score(half_q(group, half), kv[me, half, 0])
            s = jnp.where(key_no <= row_no, s, MASKED)
            m = jnp.broadcast_to(row_top(s), (tall, lanes))
            p, summed = weigh(s, m)
            write(top, half, group, m)
            write(total, half, group, summed)
            write(acc, half, group, mix(p, kv[me, half, 1]))

        over_groups(body)

    def high_on_low(owners):
        def body(group):
            keys = jnp.concatenate([kv[owner, LOW, 0] for owner in owners], axis=0)
            values = jnp.concatenate([kv[owner, LOW, 1] for owner in owners], axis=0)
            s = score(half_q(group, HIGH), keys)
            old = read(top, HIGH, group)
            m = jnp.maximum(old, row_top(s))
            fade = jnp.exp2((old - m) * scale)
            p, summed = weigh(s, m)
            write(top, HIGH, group, m)
            write(total, HIGH, group, read(total, HIGH, group) * fade + summed)
            write(acc, HIGH, group, read(acc, HIGH, group) * fade + mix(p, values))

        over_groups(body)

    def one_same_half(owner):
        flag = jnp.where(ids[2 * owner] > ids[2 * me], 1, 0)
        is_high = jnp.full((tall, lanes), flag, jnp.int32) == 1
        key_high = jnp.full((span, lanes), flag, jnp.int32) == 1
        for which in range(2):
            kv_pick[which] = jnp.where(key_high, kv[owner, HIGH, which], kv[owner, LOW, which])

        def body(group):
            s = score(jnp.where(is_high, half_q(group, HIGH), half_q(group, LOW)), kv_pick[0])
            tops = [read(top, half, group) for half in range(2)]
            old = jnp.where(is_high, tops[HIGH], tops[LOW])
            m = jnp.maximum(old, row_top(s))
            fade = jnp.exp2((old - m) * scale)
            p, summed = weigh(s, m)
            write(top, LOW, group, jnp.where(is_high, tops[LOW], m))
            write(top, HIGH, group, jnp.where(is_high, m, tops[HIGH]))
            added = mix(p, kv_pick[1])
            for ref, extra in ((total, summed), (acc, added)):
                low_now, high_now = read(ref, LOW, group), read(ref, HIGH, group)
                new = jnp.where(is_high, high_now, low_now) * fade + extra
                write(ref, LOW, group, jnp.where(is_high, low_now, new))
                write(ref, HIGH, group, jnp.where(is_high, new, high_now))

        over_groups(body)

    def same_half(owners):
        def one(index, carry):
            owner = owners[0]
            for place in range(1, len(owners)):
                owner = jnp.where(index == place, owners[place], owner)
            one_same_half(owner)
            return carry

        lax.fori_loop(0, len(owners), one, 0)

    own_span(LOW)
    own_span(HIGH)
    high_on_low((me,))

    short = jnp.minimum(z, line - 1 - z)
    far_side = jnp.where(z <= line - 1 - z, 1, -1)

    def line_place(order):
        paired = jnp.where(order % 2 == 1, -1, 1) * ((order + 1) // 2)
        alone = far_side * (order - short)
        return z + jnp.where(order <= 2 * short, paired, alone)

    def arrived(owner, half):
        sent(owner, half, TO_PARTNER).wait_recv()

    def crossed(order):
        return jnp.where(order == 0, z, line_place(order)) * 2 + 1 - x

    def visit(index, carry):
        across = crossed(index)
        along = line_place(index + 1) * 2 + x
        relay(index + 1, LOW)
        arrived(across, LOW)
        high_on_low((across, along))
        relay(index + 1, HIGH)
        arrived(across, HIGH)
        same_half((across, along))
        return carry

    lax.fori_loop(0, line - 1, visit, 0)
    last = crossed(jnp.int32(line - 1))
    arrived(last, LOW)
    high_on_low((last,))
    arrived(last, HIGH)
    same_half((last,))

    def finish(group):
        for half in range(2):
            weight = jnp.sum(total[half, group], axis=1, keepdims=True)
            out[group, half * span : (half + 1) * span, :] = (
                acc[half, group] / weight
            ).astype(out.dtype)

    def result(group):
        return pltpu.make_async_copy(
            out.at[group], o_hbm.at[:, pl.ds(group * lanes, lanes)], out_sem.at[group]
        )

    for group in range(groups):
        finish(group)
        result(group).start()

    def settle(place, carry):
        owner = place * 2 + x
        for half in range(2):
            sent(owner, half, TO_PARTNER).wait_send()

            @pl.when(jnp.logical_and(place <= z, z < line - 1))
            def _():
                sent(owner, half, TO_NEXT).wait_send()

            @pl.when(jnp.logical_and(place >= z, z > 0))
            def _():
                sent(owner, half, TO_PREV).wait_send()

        return carry

    lax.fori_loop(0, line, settle, 0)
    for group in range(groups):
        result(group).wait()


def local(count, queries, keys, values, span_ids):
    rows = queries.shape[0]
    head_dim = keys.shape[2]
    width = queries.shape[2]
    groups = width // head_dim
    span = rows // 2
    any_space = pl.BlockSpec(memory_space=pl.ANY)
    out = pl.pallas_call(
        functools.partial(kernel, count, head_dim),
        out_shape=jax.ShapeDtypeStruct((rows, width), jnp.bfloat16),
        in_specs=[pl.BlockSpec(memory_space=pltpu.SMEM), any_space, any_space, any_space],
        out_specs=any_space,
        scratch_shapes=[
            pltpu.VMEM((groups, rows, head_dim), jnp.bfloat16),
            pltpu.VMEM((count, 2, 2, span, head_dim), jnp.bfloat16),
            pltpu.VMEM((2, span, head_dim), jnp.bfloat16),
            pltpu.VMEM((2, groups, span, head_dim), jnp.float32),
            pltpu.VMEM((2, groups, span, head_dim), jnp.float32),
            pltpu.VMEM((2, groups, span, head_dim), jnp.float32),
            pltpu.VMEM((groups, rows, head_dim), jnp.bfloat16),
            pltpu.SemaphoreType.DMA((2 + groups, 2)),
            pltpu.SemaphoreType.DMA((groups,)),
            pltpu.SemaphoreType.DMA((count, 2, 3)),
            pltpu.SemaphoreType.DMA((count, 2)),
        ],
        compiler_params=pltpu.CompilerParams(
            collective_id=0, has_side_effects=True, vmem_limit_bytes=56 * 2**20
        ),
    )(
        span_ids,
        queries.reshape(rows, width),
        keys.reshape(rows, head_dim),
        values.reshape(rows, head_dim),
    )
    return out.reshape(rows, 1, width)


def solution(mesh):
    in_specs = (P("ctx", "head", None), P("ctx", "head", None), P("ctx", "head", None), P())
    out_specs = P("ctx", "head", None)
    body = functools.partial(local, mesh.shape["ctx"])
    return jax.shard_map(body, mesh=mesh, in_specs=in_specs, out_specs=out_specs, check_vma=False)
```
